32 devices in a mesh: gx: 4 (over z), gy: 4 (over x, core), gz: 2 (over y).
Axes of the slice: x: 2, y: 2, z: 4, core: 2. Of those that a mesh axis runs over, the one named last changes fastest.
Arguments:
- volume: int32 [32, 64, 256], P('gx', 'gy', 'gz'), may hold values from 0 to 255
- transfer_table: float32 [4, 256], replicated, may hold values from 0 to 1
- depth_rank: int32 [4], replicated, may hold values from 0 to 3, each once
- footprint: int32 [4, 4, 2, 4], P('gx', 'gy', 'gz'), may hold values from 0 to 128, as said below
Outputs:
- rendered: float32 [4, 64, 256], P(None, 'gy', 'gz')
The draws below stay inside these ranges and needn't reach their ends.
Inputs may be any that keep to these rules, and one draw needn't show every extreme that they name: depth_rank holds each of 0 to 4 - 1 once. `footprint`: for every brick, entry 0 is below 8 and entry 1 above it, up to 16; entry 2 is below 64 and entry 3 above it, up to 128.
All inputs are finite; a program needn't handle non-finite values.
Results may differ from the reference program's by a relative error of at most 0.0003.
Values sent between devices are 32-bit elements; how exact they have to be, the bound alone decides.
A program may use at most 64 MiB of HBM per device.

```python
import jax
import jax.numpy as jnp
from jax import lax

CX = 8
CY = 16
CZ = 128
TF = 256
NX = 32
NY = 64
NZ = 256
N_GX = 4
N_GY = 4
N_GZ = 2


def draw_footprint(key, part):
    keys = jax.random.split(jax.random.fold_in(key, 7), 4)
    shaped = (N_GX, N_GY, N_GZ)
    first_row = jax.random.randint(keys[0], shaped, 0, CY // 2)
    end_row = jax.random.randint(keys[1], shaped, CY // 2 + 1, CY + 1)
    first_col = jax.random.randint(keys[2], shaped, 0, CZ // 2)
    end_col = jax.random.randint(keys[3], shaped, CZ // 2 + 1, CZ + 1)
    return jnp.stack([first_row, end_row, first_col, end_col], axis=-1).astype(jnp.int32)


def with_ends(result, stream_key, least, high):
    longest = result.shape.index(max(result.shape))
    spots = []
    for shift in (0, 1):
        where = [jax.random.randint(jax.random.fold_in(stream_key, axis), (), 0, length) for axis, length in enumerate(result.shape)]
        where[longest] = (where[longest] + shift) % result.shape[longest]
        spots.append(tuple(where))
    return result.at[spots[0]].set(least).at[spots[1]].set(high)


def setup_inputs(seed: int = 0) -> dict:
    key_list = jax.random.split(jax.random.key(seed), 5)
    return {
        "volume": with_ends(jax.random.randint(key_list[0], (NX, NY, NZ), 0, TF), jax.random.fold_in(key_list[0], 1), 0, TF - 1).astype(jnp.int32),
        "transfer_table": jnp.clip(jax.random.uniform(key_list[1], (4, TF), jnp.float32, 0.0, 1.0), 0.0, 1.0),
        "depth_rank": jax.random.permutation(key_list[2], N_GX).astype(jnp.int32),
        "footprint": draw_footprint(jax.random.fold_in(key_list[4], 71), 0),
    }


light_x = 1.0 / 3.0
light_y = 2.0 / 3.0
light_z = 2.0 / 3.0

def shading(lower_plane, upper_plane, padded):
    grad_x = 0.5 * (upper_plane - lower_plane)
    grad_y = 0.5 * (padded[2:, 1:-1] - padded[:-2, 1:-1])
    grad_z = 0.5 * (padded[1:-1, 2:] - padded[1:-1, :-2])
    facing = jnp.abs(grad_x * light_x + grad_y * light_y + grad_z * light_z) / jnp.sqrt(1.0 + (grad_x * grad_x + grad_y * grad_y + grad_z * grad_z))
    return 0.35 + 0.65 * facing

def composite(layers, depth_rank):
    order = jnp.argsort(depth_rank).astype(jnp.int32)
    ordered = jnp.take(layers, order, axis=0)

    def blend(state_pair, front_layer):
        colour, alpha = state_pair
        cover = 1.0 - alpha
        return ((colour + cover * front_layer[:3], alpha + cover * front_layer[3]), None)
    start_pair = (jnp.zeros((3,) + layers.shape[2:], jnp.float32), jnp.zeros(layers.shape[2:], jnp.float32))
    (colour, alpha), unused = lax.scan(blend, start_pair, ordered)
    return jnp.concatenate([colour, alpha[None]], axis=0)

def reference(volume, transfer_table, depth_rank, footprint):
    opacity = transfer_table[3]
    colors = transfer_table[:3]
    extent = 4.0 / NX

    def density(slice_at):
        inside = ((slice_at >= 0) & (slice_at < NX)).astype(jnp.float32)
        clipped = jnp.clip(slice_at, 0, NX - 1).astype(jnp.int32)
        indices = lax.dynamic_index_in_dim(volume, clipped, 0, keepdims=False)
        return (jnp.take(opacity, indices, axis=0) * inside, indices)

    def advance(state_pair, slice_at):
        colour, transmit = state_pair
        centre, indices = density(slice_at)
        lower_plane, unused_low = density(slice_at - 1)
        upper_plane, unused_high = density(slice_at + 1)
        shading_term = shading(lower_plane, upper_plane, jnp.pad(centre, 1))
        emitted = jnp.take(colors, indices, axis=1) * shading_term
        sample_alpha = 1.0 - jnp.exp(-extent * centre)
        colour = colour + transmit * sample_alpha * emitted
        transmit = transmit * (1.0 - sample_alpha)
        return ((colour, transmit), None)
    rows_local = (jnp.arange(NY, dtype=jnp.int32) % CY)[:, None]
    cols_local = (jnp.arange(NZ, dtype=jnp.int32) % CZ)[None, :]
    partials = []
    for column in range(N_GX):
        start_pair = (jnp.zeros((3, NY, NZ), jnp.float32), jnp.ones((NY, NZ), jnp.float32))
        slices_here = jnp.arange(CX, dtype=jnp.int32) + column * CX
        (colour, transmit), unused = lax.scan(advance, start_pair, slices_here)
        rect = jnp.repeat(jnp.repeat(footprint[column], CY, axis=0), CZ, axis=1)
        inside = (rows_local >= rect[..., 0]) & (rows_local < rect[..., 1]) & (cols_local >= rect[..., 2]) & (cols_local < rect[..., 3])
        layer = jnp.concatenate([colour, (1.0 - transmit)[None]], axis=0)
        partials.append(jnp.where(inside[None], layer, 0.0))
    return composite(jnp.stack(partials), depth_rank)
```

```python
import functools

import jax
import jax.numpy as jnp
from jax import lax
from jax.experimental import pallas as pl
from jax.experimental.pallas import tpu as pltpu
from jax.sharding import PartitionSpec as P

LIGHT = (1.0 / 3.0, 2.0 / 3.0, 2.0 / 3.0)
AXES = ("gx", "gy", "gz")
MESH = pl.DeviceIdType.MESH


def lookup(table_row, index, lanes):
    entries = table_row.shape[1]
    low = index & (lanes - 1)
    found = None
    for part in range(entries // lanes):
        piece = jnp.broadcast_to(table_row[:, part * lanes:(part + 1) * lanes], index.shape)
        got = jnp.take_along_axis(piece, low, axis=1, mode="promise_in_bounds")
        found = got if found is None else jnp.where(index >= part * lanes, got, found)
    return found


def kernel(sizes, vol_ref, table_ref, rank_ref, foot_ref, out_ref,
           dens, wemit, edge, xh, yh, zh, alphas, colours,
           halo_send, halo_recv, a_send, a_recv, c_send, c_recv):
    n, ny, nz = sizes
    depth, rows, lanes = vol_ref.shape
    extent = 4.0 / (depth * n)
    me = [lax.axis_index(a) for a in AXES]
    ix = me[0]

    barrier = pltpu.get_barrier_semaphore()
    for off in range(1, n):
        pl.semaphore_signal(barrier, inc=1, device_id={"gx": lax.rem(ix + off, n)}, device_id_type=MESH)
    for a in (1, 2):
        if sizes[a] > 1:
            @pl.when(me[a] > 0)
            def _():
                pl.semaphore_signal(barrier, inc=1, device_id={AXES[a]: me[a] - 1}, device_id_type=MESH)

            @pl.when(me[a] < sizes[a] - 1)
            def _():
                pl.semaphore_signal(barrier, inc=1, device_id={AXES[a]: me[a] + 1}, device_id_type=MESH)

    lane = lax.broadcasted_iota(jnp.int32, (8, lanes), 1)
    vol = vol_ref[...].reshape(depth * rows, lanes)
    d_all = lookup(table_ref[3:4, :], vol, lanes)
    d3 = d_all.reshape(depth, rows, lanes)
    dens[...] = d3
    edge[0] = d3[:, 0, :]
    edge[1] = d3[:, rows - 1, :]
    first = jnp.zeros((8, lanes), jnp.float32)
    last = jnp.zeros((8, lanes), jnp.float32)
    groups = depth * rows // 8
    for v in range(groups):
        piece = d_all[v * 8:(v + 1) * 8]
        to_last = (2 * v + 1) % lanes
        to_first = (2 * v - 1) % lanes
        last = jnp.where(lane == 2 * v, pltpu.roll(piece, to_last, 1) if to_last else piece, last)
        first = jnp.where(lane == to_first, pltpu.roll(piece, to_first, 1) if to_first else piece, first)
    edge[2] = first
    edge[3] = last

    sources = (
        (dens.at[0], dens.at[depth - 1]),
        (edge.at[0], edge.at[1]),
        (edge.at[2], edge.at[3]),
    )
    halos = (xh, yh, zh)

    def halo_copy(a, upward):
        slot = 0 if upward else 1
        return pltpu.make_async_remote_copy(
            src_ref=sources[a][1 if upward else 0],
            dst_ref=halos[a].at[slot],
            send_sem=halo_send.at[a, slot],
            recv_sem=halo_recv.at[a, slot],
            device_id={AXES[a]: me[a] + (1 if upward else -1)},
            device_id_type=MESH,
        )

    greeted = n - 1
    for a in (1, 2):
        greeted = greeted + lax.min(me[a], 1) + lax.min(sizes[a] - 1 - me[a], 1)
    pl.semaphore_wait(barrier, greeted)

    for a in range(3):
        @pl.when(me[a] < sizes[a] - 1)
        def _():
            halo_copy(a, True).start()

        @pl.when(me[a] == 0)
        def _():
            halos[a][0] = jnp.zeros(halos[a].shape[1:], jnp.float32)

        @pl.when(me[a] > 0)
        def _():
            halo_copy(a, False).start()

        @pl.when(me[a] == sizes[a] - 1)
        def _():
            halos[a][1] = jnp.zeros(halos[a].shape[1:], jnp.float32)

    row_no = lax.broadcasted_iota(jnp.int32, (rows, lanes), 0)
    lane_no = lax.broadcasted_iota(jnp.int32, (rows, lanes), 1)
    inside = (
        (row_no >= foot_ref[0, 0, 0, 0])
        & (row_no < foot_ref[0, 0, 0, 1])
        & (lane_no >= foot_ref[0, 0, 0, 2])
        & (lane_no < foot_ref[0, 0, 0, 3])
    )

    transmit = jnp.ones((rows, lanes), jnp.float32)
    weights = []
    for x in range(depth):
        sample = 1.0 - jnp.exp(-extent * d3[x])
        weights.append(transmit * sample)
        transmit = transmit * (1.0 - sample)
    alphas[ix] = jnp.where(inside, 1.0 - transmit, 0.0)

    def image_copy(buf, off, s_sem, r_sem):
        return pltpu.make_async_remote_copy(
            src_ref=buf.at[ix],
            dst_ref=buf.at[ix],
            send_sem=s_sem.at[off],
            recv_sem=r_sem.at[off],
            device_id={"gx": lax.rem(ix + off, n)},
            device_id_type=MESH,
        )

    for off in range(n - 1, 0, -1):
        image_copy(alphas, off, a_send, a_recv).start()

    for c in range(3):
        emit = lookup(table_ref[c:c + 1, :], vol, lanes).reshape(depth, rows, lanes)
        for x in range(depth):
            wemit[c, x] = weights[x] * emit[x]

    for a in range(3):
        @pl.when(me[a] > 0)
        def _():
            halo_copy(a, True).wait_recv()

        @pl.when(me[a] < sizes[a] - 1)
        def _():
            halo_copy(a, False).wait_recv()

    sides = zh[0] + zh[1]
    layers = [xh[0]] + [dens[x] for x in range(depth)] + [xh[1]]
    colour = [jnp.zeros((rows, lanes), jnp.float32) for _ in range(3)]
    per = rows // 8
    for x in range(depth):
        d = layers[x + 1]
        g_x = 0.5 * (layers[x + 2] - layers[x])
        up = jnp.where(row_no == 0, yh[0, x:x + 1, :], pltpu.roll(d, 1, 0))
        down = jnp.where(row_no == rows - 1, yh[1, x:x + 1, :], pltpu.roll(d, rows - 1, 0))
        g_y = 0.5 * (down - up)
        pieces = []
        for h in range(per):
            v = x * per + h
            pieces.append(pltpu.roll(sides, (lanes - 2 * v) % lanes, 1) if v else sides)
        side = jnp.concatenate(pieces, axis=0)
        left = jnp.where(lane_no == 0, side, pltpu.roll(d, 1, 1))
        right = jnp.where(lane_no == lanes - 1, side, pltpu.roll(d, lanes - 1, 1))
        g_z = 0.5 * (right - left)
        facing = jnp.abs(g_x * LIGHT[0] + g_y * LIGHT[1] + g_z * LIGHT[2]) * lax.rsqrt(
            1.0 + (g_x * g_x + g_y * g_y + g_z * g_z)
        )
        shade = 0.35 + 0.65 * facing
        for c in range(3):
            colour[c] = colour[c] + wemit[c, x] * shade
    for c in range(3):
        colours[ix, c] = jnp.where(inside, colour[c], 0.0)

    for off in range(n - 1, 0, -1):
        image_copy(colours, off, c_send, c_recv).start()

    order = []
    for p in range(n):
        at = 0
        for i in range(n):
            at = jnp.where(rank_ref[i] == p, i, at)
        order.append(at)

    for off in range(1, n):
        image_copy(alphas, off, a_send, a_recv).wait_recv()
    for off in range(1, n):
        image_copy(colours, off, c_send, c_recv).wait_recv()

    total = [jnp.zeros((rows, lanes), jnp.float32) for _ in range(4)]
    for p in range(n):
        cover = 1.0 - total[3]
        for c in range(3):
            total[c] = total[c] + cover * colours[order[p], c]
        total[3] = total[3] + cover * alphas[order[p]]
    for c in range(4):
        out_ref[c] = total[c]

    for a in range(3):
        @pl.when(me[a] < sizes[a] - 1)
        def _():
            halo_copy(a, True).wait_send()

        @pl.when(me[a] > 0)
        def _():
            halo_copy(a, False).wait_send()
    for off in range(1, n):
        image_copy(alphas, off, a_send, a_recv).wait_send()
        image_copy(colours, off, c_send, c_recv).wait_send()


def on_device(sizes, volume, transfer_table, depth_rank, footprint):
    depth, rows, lanes = volume.shape
    n = sizes[0]
    vmem = pl.BlockSpec(memory_space=pltpu.VMEM)
    smem = pl.BlockSpec(memory_space=pltpu.SMEM)
    return pl.pallas_call(
        functools.partial(kernel, sizes),
        out_shape=jax.ShapeDtypeStruct((4, rows, lanes), jnp.float32),
        in_specs=[vmem, vmem, smem, smem],
        out_specs=vmem,
        scratch_shapes=[
            pltpu.VMEM((depth, rows, lanes), jnp.float32),
            pltpu.VMEM((3, depth, rows, lanes), jnp.float32),
            pltpu.VMEM((4, 8, lanes), jnp.float32),
            pltpu.VMEM((2, rows, lanes), jnp.float32),
            pltpu.VMEM((2, depth, lanes), jnp.float32),
            pltpu.VMEM((2, 8, lanes), jnp.float32),
            pltpu.VMEM((n, rows, lanes), jnp.float32),
            pltpu.VMEM((n, 3, rows, lanes), jnp.float32),
            pltpu.SemaphoreType.DMA((3, 2)),
            pltpu.SemaphoreType.DMA((3, 2)),
            pltpu.SemaphoreType.DMA((n,)),
            pltpu.SemaphoreType.DMA((n,)),
            pltpu.SemaphoreType.DMA((n,)),
            pltpu.SemaphoreType.DMA((n,)),
        ],
        compiler_params=pltpu.CompilerParams(collective_id=0, has_side_effects=True),
        name="raycast",
    )(volume, transfer_table, depth_rank, footprint)


def solution(mesh):
    placed = (P("gx", "gy", "gz"), P(), P(), P("gx", "gy", "gz", None))
    sizes = tuple(mesh.shape[a] for a in AXES)
    return jax.shard_map(
        functools.partial(on_device, sizes), mesh=mesh, in_specs=placed,
        out_specs=P(None, "gy", "gz"), check_vma=False,
    )
```

```python
import functools

import jax
import jax.numpy as jnp
from jax import lax
from jax.experimental import pallas as pl
from jax.experimental.pallas import tpu as pltpu
from jax.sharding import PartitionSpec as P

LIGHT = (1.0 / 3.0, 2.0 / 3.0, 2.0 / 3.0)
AXES = ("gx", "gy", "gz")
MESH = pl.DeviceIdType.MESH


def lookup(table_row, index, lanes):
    entries = table_row.shape[1]
    low = index & (lanes - 1)
    found = None
    for part in range(entries // lanes):
        piece = jnp.broadcast_to(table_row[:, part * lanes:(part + 1) * lanes], index.shape)
        got = jnp.take_along_axis(piece, low, axis=1, mode="promise_in_bounds")
        found = got if found is None else jnp.where(index >= part * lanes, got, found)
    return found


def kernel(sizes, vol_hbm, table_hbm, rank_hbm, foot_hbm, out_ref,
           vol_ref, table_ref, rank_ref, foot_ref, load_sem, dens, wemit, edge, xh, yh, zh, alphas, colours,
           halo_send, halo_recv, a_send, a_recv, c_send, c_recv):
    n, ny, nz = sizes
    depth, rows, lanes = vol_ref.shape
    extent = 4.0 / (depth * n)
    me = [lax.axis_index(a) for a in AXES]
    ix = me[0]

    barrier = pltpu.get_barrier_semaphore()
    for off in range(1, n):
        pl.semaphore_signal(barrier, inc=1, device_id={"gx": lax.rem(ix + off, n)}, device_id_type=MESH)
    for a in (1, 2):
        if sizes[a] > 1:
            @pl.when(me[a] > 0)
            def _():
                pl.semaphore_signal(barrier, inc=1, device_id={AXES[a]: me[a] - 1}, device_id_type=MESH)

            @pl.when(me[a] < sizes[a] - 1)
            def _():
                pl.semaphore_signal(barrier, inc=1, device_id={AXES[a]: me[a] + 1}, device_id_type=MESH)

    loads = [
        pltpu.make_async_copy(src, dst, load_sem.at[i])
        for i, (src, dst) in enumerate((
            (vol_hbm, vol_ref), (table_hbm, table_ref), (foot_hbm, foot_ref), (rank_hbm, rank_ref)
        ))
    ]
    for load in loads:
        load.start()
    loads[0].wait()
    loads[1].wait()

    lane = lax.broadcasted_iota(jnp.int32, (8, lanes), 1)
    vol = vol_ref[...].reshape(depth * rows, lanes)
    d_all = lookup(table_ref[3:4, :], vol, lanes)
    d3 = d_all.reshape(depth, rows, lanes)
    dens[...] = d3
    edge[0] = d3[:, 0, :]
    edge[1] = d3[:, rows - 1, :]
    first = jnp.zeros((8, lanes), jnp.float32)
    last = jnp.zeros((8, lanes), jnp.float32)
    groups = depth * rows // 8
    for v in range(groups):
        piece = d_all[v * 8:(v + 1) * 8]
        to_last = (2 * v + 1) % lanes
        to_first = (2 * v - 1) % lanes
        last = jnp.where(lane == 2 * v, pltpu.roll(piece, to_last, 1) if to_last else piece, last)
        first = jnp.where(lane == to_first, pltpu.roll(piece, to_first, 1) if to_first else piece, first)
    edge[2] = first
    edge[3] = last

    sources = (
        (dens.at[0], dens.at[depth - 1]),
        (edge.at[0], edge.at[1]),
        (edge.at[2], edge.at[3]),
    )
    halos = (xh, yh, zh)

    def halo_copy(a, upward):
        slot = 0 if upward else 1
        return pltpu.make_async_remote_copy(
            src_ref=sources[a][1 if upward else 0],
            dst_ref=halos[a].at[slot],
            send_sem=halo_send.at[a, slot],
            recv_sem=halo_recv.at[a, slot],
            device_id={AXES[a]: me[a] + (1 if upward else -1)},
            device_id_type=MESH,
        )

    greeted = n - 1
    for a in (1, 2):
        greeted = greeted + lax.min(me[a], 1) + lax.min(sizes[a] - 1 - me[a], 1)
    pl.semaphore_wait(barrier, greeted)

    for a in range(3):
        @pl.when(me[a] < sizes[a] - 1)
        def _():
            halo_copy(a, True).start()

        @pl.when(me[a] == 0)
        def _():
            halos[a][0] = jnp.zeros(halos[a].shape[1:], jnp.float32)

        @pl.when(me[a] > 0)
        def _():
            halo_copy(a, False).start()

        @pl.when(me[a] == sizes[a] - 1)
        def _():
            halos[a][1] = jnp.zeros(halos[a].shape[1:], jnp.float32)

    loads[2].wait()
    row_no = lax.broadcasted_iota(jnp.int32, (rows, lanes), 0)
    lane_no = lax.broadcasted_iota(jnp.int32, (rows, lanes), 1)
    inside = (
        (row_no >= foot_ref[0, 0, 0, 0])
        & (row_no < foot_ref[0, 0, 0, 1])
        & (lane_no >= foot_ref[0, 0, 0, 2])
        & (lane_no < foot_ref[0, 0, 0, 3])
    )

    transmit = jnp.ones((rows, lanes), jnp.float32)
    weights = []
    for x in range(depth):
        sample = 1.0 - jnp.exp(-extent * d3[x])
        weights.append(transmit * sample)
        transmit = transmit * (1.0 - sample)
    alphas[ix] = jnp.where(inside, 1.0 - transmit, 0.0)

    def image_copy(buf, off, s_sem, r_sem):
        return pltpu.make_async_remote_copy(
            src_ref=buf.at[ix],
            dst_ref=buf.at[ix],
            send_sem=s_sem.at[off],
            recv_sem=r_sem.at[off],
            device_id={"gx": lax.rem(ix + off, n)},
            device_id_type=MESH,
        )

    def send_images(buf, s_sem, r_sem):
        for far in range(n - 1, 0, -1):
            @pl.when(ix + far < n)
            def _():
                image_copy(buf, far, s_sem, r_sem).start()

            @pl.when(ix - far >= 0)
            def _():
                image_copy(buf, n - far, s_sem, r_sem).start()

    send_images(alphas, a_send, a_recv)

    for c in range(3):
        emit = lookup(table_ref[c:c + 1, :], vol, lanes).reshape(depth, rows, lanes)
        for x in range(depth):
            wemit[c, x] = weights[x] * emit[x]

    for a in range(3):
        @pl.when(me[a] > 0)
        def _():
            halo_copy(a, True).wait_recv()

        @pl.when(me[a] < sizes[a] - 1)
        def _():
            halo_copy(a, False).wait_recv()

    sides = zh[0] + zh[1]
    layers = [xh[0]] + [dens[x] for x in range(depth)] + [xh[1]]
    colour = [jnp.zeros((rows, lanes), jnp.float32) for _ in range(3)]
    per = rows // 8
    for x in range(depth):
        d = layers[x + 1]
        g_x = 0.5 * (layers[x + 2] - layers[x])
        up = jnp.where(row_no == 0, yh[0, x:x + 1, :], pltpu.roll(d, 1, 0))
        down = jnp.where(row_no == rows - 1, yh[1, x:x + 1, :], pltpu.roll(d, rows - 1, 0))
        g_y = 0.5 * (down - up)
        pieces = []
        for h in range(per):
            v = x * per + h
            pieces.append(pltpu.roll(sides, (lanes - 2 * v) % lanes, 1) if v else sides)
        side = jnp.concatenate(pieces, axis=0)
        left = jnp.where(lane_no == 0, side, pltpu.roll(d, 1, 1))
        right = jnp.where(lane_no == lanes - 1, side, pltpu.roll(d, lanes - 1, 1))
        g_z = 0.5 * (right - left)
        facing = jnp.abs(g_x * LIGHT[0] + g_y * LIGHT[1] + g_z * LIGHT[2]) * lax.rsqrt(
            1.0 + (g_x * g_x + g_y * g_y + g_z * g_z)
        )
        shade = 0.35 + 0.65 * facing
        for c in range(3):
            colour[c] = colour[c] + wemit[c, x] * shade
    for c in range(3):
        colours[ix, c] = jnp.where(inside, colour[c], 0.0)

    send_images(colours, c_send, c_recv)

    loads[3].wait()
    order = []
    for p in range(n):
        at = 0
        for i in range(n):
            at = jnp.where(rank_ref[i] == p, i, at)
        order.append(at)

    for off in range(1, n):
        image_copy(alphas, off, a_send, a_recv).wait_recv()
    for off in range(1, n):
        image_copy(colours, off, c_send, c_recv).wait_recv()

    total = [jnp.zeros((rows, lanes), jnp.float32) for _ in range(4)]
    for p in range(n):
        cover = 1.0 - total[3]
        for c in range(3):
            total[c] = total[c] + cover * colours[order[p], c]
        total[3] = total[3] + cover * alphas[order[p]]
    for c in range(4):
        out_ref[c] = total[c]

    for a in range(3):
        @pl.when(me[a] < sizes[a] - 1)
        def _():
            halo_copy(a, True).wait_send()

        @pl.when(me[a] > 0)
        def _():
            halo_copy(a, False).wait_send()
    for off in range(1, n):
        image_copy(alphas, off, a_send, a_recv).wait_send()
        image_copy(colours, off, c_send, c_recv).wait_send()


def on_device(sizes, volume, transfer_table, depth_rank, footprint):
    depth, rows, lanes = volume.shape
    n = sizes[0]
    vmem = pl.BlockSpec(memory_space=pltpu.VMEM)
    hbm = pl.BlockSpec(memory_space=pl.ANY)
    return pl.pallas_call(
        functools.partial(kernel, sizes),
        out_shape=jax.ShapeDtypeStruct((4, rows, lanes), jnp.float32),
        in_specs=[hbm] * 4,
        out_specs=vmem,
        scratch_shapes=[
            pltpu.VMEM(volume.shape, jnp.int32),
            pltpu.VMEM(transfer_table.shape, jnp.float32),
            pltpu.SMEM(depth_rank.shape, jnp.int32),
            pltpu.SMEM(footprint.shape, jnp.int32),
            pltpu.SemaphoreType.DMA((4,)),
            pltpu.VMEM((depth, rows, lanes), jnp.float32),
            pltpu.VMEM((3, depth, rows, lanes), jnp.float32),
            pltpu.VMEM((4, 8, lanes), jnp.float32),
            pltpu.VMEM((2, rows, lanes), jnp.float32),
            pltpu.VMEM((2, depth, lanes), jnp.float32),
            pltpu.VMEM((2, 8, lanes), jnp.float32),
            pltpu.VMEM((n, rows, lanes), jnp.float32),
            pltpu.VMEM((n, 3, rows, lanes), jnp.float32),
            pltpu.SemaphoreType.DMA((3, 2)),
            pltpu.SemaphoreType.DMA((3, 2)),
            pltpu.SemaphoreType.DMA((n,)),
            pltpu.SemaphoreType.DMA((n,)),
            pltpu.SemaphoreType.DMA((n,)),
            pltpu.SemaphoreType.DMA((n,)),
        ],
        compiler_params=pltpu.CompilerParams(collective_id=0, has_side_effects=True),
        name="raycast",
    )(volume, transfer_table, depth_rank, footprint)


def solution(mesh):
    placed = (P("gx", "gy", "gz"), P(), P(), P("gx", "gy", "gz", None))
    sizes = tuple(mesh.shape[a] for a in AXES)
    return jax.shard_map(
        functools.partial(on_device, sizes), mesh=mesh, in_specs=placed,
        out_specs=P(None, "gy", "gz"), check_vma=False,
    )
```

```python
import functools

import jax
import jax.numpy as jnp
from jax import lax
from jax.experimental import pallas as pl
from jax.experimental.pallas import tpu as pltpu
from jax.sharding import PartitionSpec as P

LIGHT = (1.0 / 3.0, 2.0 / 3.0, 2.0 / 3.0)
AXES = ("gx", "gy", "gz")
MESH = pl.DeviceIdType.MESH


def lookup(table_row, index, lanes):
    entries = table_row.shape[1]
    low = index & (lanes - 1)
    found = None
    for part in range(entries // lanes):
        piece = jnp.broadcast_to(table_row[:, part * lanes:(part + 1) * lanes], index.shape)
        got = jnp.take_along_axis(piece, low, axis=1, mode="promise_in_bounds")
        found = got if found is None else jnp.where(index >= part * lanes, got, found)
    return found


def kernel(sizes, vol_hbm, table_hbm, rank_hbm, foot_hbm, out_ref,
           vol_ref, table_ref, rank_ref, foot_ref, load_sem, dens, wemit, edge, xh, yh, zh, alphas, colours,
           halo_send, halo_recv, a_send, a_recv, c_send, c_recv):
    n, ny, nz = sizes
    depth, rows, lanes = vol_ref.shape
    extent = 4.0 / (depth * n)
    me = [lax.axis_index(a) for a in AXES]
    ix = me[0]

    barrier = pltpu.get_barrier_semaphore()
    for off in range(1, n):
        pl.semaphore_signal(barrier, inc=1, device_id={"gx": lax.rem(ix + off, n)}, device_id_type=MESH)
    for a in (1, 2):
        if sizes[a] > 1:
            @pl.when(me[a] > 0)
            def _():
                pl.semaphore_signal(barrier, inc=1, device_id={AXES[a]: me[a] - 1}, device_id_type=MESH)

            @pl.when(me[a] < sizes[a] - 1)
            def _():
                pl.semaphore_signal(barrier, inc=1, device_id={AXES[a]: me[a] + 1}, device_id_type=MESH)

    loads = [
        pltpu.make_async_copy(src, dst, load_sem.at[i])
        for i, (src, dst) in enumerate((
            (vol_hbm, vol_ref), (table_hbm, table_ref), (foot_hbm, foot_ref), (rank_hbm, rank_ref)
        ))
    ]
    for load in loads:
        load.start()
    loads[0].wait()
    loads[1].wait()

    lane = lax.broadcasted_iota(jnp.int32, (8, lanes), 1)
    vol = vol_ref[...].reshape(depth * rows, lanes)
    d_all = lookup(table_ref[3:4, :], vol, lanes)
    d3 = d_all.reshape(depth, rows, lanes)
    dens[...] = d3
    edge[0] = d3[:, 0, :]
    edge[1] = d3[:, rows - 1, :]
    first = jnp.zeros((8, lanes), jnp.float32)
    last = jnp.zeros((8, lanes), jnp.float32)
    groups = depth * rows // 8
    for v in range(groups):
        piece = d_all[v * 8:(v + 1) * 8]
        to_last = (2 * v + 1) % lanes
        to_first = (2 * v - 1) % lanes
        last = jnp.where(lane == 2 * v, pltpu.roll(piece, to_last, 1) if to_last else piece, last)
        first = jnp.where(lane == to_first, pltpu.roll(piece, to_first, 1) if to_first else piece, first)
    edge[2] = first
    edge[3] = last

    sources = (
        (dens.at[0], dens.at[depth - 1]),
        (edge.at[0], edge.at[1]),
        (edge.at[2], edge.at[3]),
    )
    halos = (xh, yh, zh)

    def halo_copy(a, upward):
        slot = 0 if upward else 1
        return pltpu.make_async_remote_copy(
            src_ref=sources[a][1 if upward else 0],
            dst_ref=halos[a].at[slot],
            send_sem=halo_send.at[a, slot],
            recv_sem=halo_recv.at[a, slot],
            device_id={AXES[a]: me[a] + (1 if upward else -1)},
            device_id_type=MESH,
        )

    greeted = n - 1
    for a in (1, 2):
        greeted = greeted + lax.min(me[a], 1) + lax.min(sizes[a] - 1 - me[a], 1)
    pl.semaphore_wait(barrier, greeted)

    for a in range(3):
        @pl.when(me[a] < sizes[a] - 1)
        def _():
            halo_copy(a, True).start()

        @pl.when(me[a] == 0)
        def _():
            halos[a][0] = jnp.zeros(halos[a].shape[1:], jnp.float32)

        @pl.when(me[a] > 0)
        def _():
            halo_copy(a, False).start()

        @pl.when(me[a] == sizes[a] - 1)
        def _():
            halos[a][1] = jnp.zeros(halos[a].shape[1:], jnp.float32)

    loads[2].wait()
    row_no = lax.broadcasted_iota(jnp.int32, (rows, lanes), 0)
    lane_no = lax.broadcasted_iota(jnp.int32, (rows, lanes), 1)
    inside = (
        (row_no >= foot_ref[0, 0, 0, 0])
        & (row_no < foot_ref[0, 0, 0, 1])
        & (lane_no >= foot_ref[0, 0, 0, 2])
        & (lane_no < foot_ref[0, 0, 0, 3])
    )

    transmit = jnp.ones((rows, lanes), jnp.float32)
    weights = []
    for x in range(depth):
        sample = 1.0 - jnp.exp(-extent * d3[x])
        weights.append(transmit * sample)
        transmit = transmit * (1.0 - sample)
    alphas[ix] = jnp.where(inside, 1.0 - transmit, 0.0)

    def image_copy(buf, off, s_sem, r_sem):
        return pltpu.make_async_remote_copy(
            src_ref=buf.at[ix],
            dst_ref=buf.at[ix],
            send_sem=s_sem.at[off],
            recv_sem=r_sem.at[off],
            device_id={"gx": lax.rem(ix + off, n)},
            device_id_type=MESH,
        )

    def send_images(buf, s_sem, r_sem):
        for far in range(n - 1, 0, -1):
            @pl.when(ix + far < n)
            def _():
                image_copy(buf, far, s_sem, r_sem).start()

            @pl.when(ix - far >= 0)
            def _():
                image_copy(buf, n - far, s_sem, r_sem).start()

    send_images(alphas, a_send, a_recv)

    for c in range(3):
        emit = lookup(table_ref[c:c + 1, :], vol, lanes).reshape(depth, rows, lanes)
        for x in range(depth):
            wemit[c, x] = weights[x] * emit[x]

    for a in range(3):
        @pl.when(me[a] > 0)
        def _():
            halo_copy(a, True).wait_recv()

        @pl.when(me[a] < sizes[a] - 1)
        def _():
            halo_copy(a, False).wait_recv()

    sides = zh[0] + zh[1]
    layers = [xh[0]] + [dens[x] for x in range(depth)] + [xh[1]]
    colour = [jnp.zeros((rows, lanes), jnp.float32) for _ in range(3)]
    per = rows // 8
    for x in range(depth):
        d = layers[x + 1]
        g_x = 0.5 * (layers[x + 2] - layers[x])
        up = jnp.where(row_no == 0, yh[0, x:x + 1, :], pltpu.roll(d, 1, 0))
        down = jnp.where(row_no == rows - 1, yh[1, x:x + 1, :], pltpu.roll(d, rows - 1, 0))
        g_y = 0.5 * (down - up)
        pieces = []
        for h in range(per):
            v = x * per + h
            pieces.append(pltpu.roll(sides, (lanes - 2 * v) % lanes, 1) if v else sides)
        side = jnp.concatenate(pieces, axis=0)
        left = jnp.where(lane_no == 0, side, pltpu.roll(d, 1, 1))
        right = jnp.where(lane_no == lanes - 1, side, pltpu.roll(d, lanes - 1, 1))
        g_z = 0.5 * (right - left)
        facing = jnp.abs(g_x * LIGHT[0] + g_y * LIGHT[1] + g_z * LIGHT[2]) * lax.rsqrt(
            1.0 + (g_x * g_x + g_y * g_y + g_z * g_z)
        )
        shade = 0.35 + 0.65 * facing
        for c in range(3):
            colour[c] = colour[c] + wemit[c, x] * shade
    for c in range(3):
        colours[ix, c] = jnp.where(inside, colour[c], 0.0)

    send_images(colours, c_send, c_recv)

    loads[3].wait()
    order = []
    for p in range(n):
        at = 0
        for i in range(n):
            at = jnp.where(rank_ref[i] == p, i, at)
        order.append(at)

    for off in range(1, n):
        image_copy(alphas, off, a_send, a_recv).wait_recv()
    for off in range(1, n):
        image_copy(colours, off, c_send, c_recv).wait_recv()

    total = [jnp.zeros((rows, lanes), jnp.float32) for _ in range(4)]
    for p in range(n):
        cover = 1.0 - total[3]
        for c in range(3):
            total[c] = total[c] + cover * colours[order[p], c]
        total[3] = total[3] + cover * alphas[order[p]]
    for c in range(4):
        out_ref[c] = total[c]

    for a in range(3):
        @pl.when(me[a] < sizes[a] - 1)
        def _():
            halo_copy(a, True).wait_send()

        @pl.when(me[a] > 0)
        def _():
            halo_copy(a, False).wait_send()
    for off in range(1, n):
        image_copy(alphas, off, a_send, a_recv).wait_send()
        image_copy(colours, off, c_send, c_recv).wait_send()


def on_device(sizes, volume, transfer_table, depth_rank, footprint):
    depth, rows, lanes = volume.shape
    n = sizes[0]
    vmem = pl.BlockSpec(memory_space=pltpu.VMEM)
    hbm = pl.BlockSpec(memory_space=pl.ANY)
    return pl.pallas_call(
        functools.partial(kernel, sizes),
        out_shape=pltpu.VMEM((4, rows, lanes), jnp.float32),
        in_specs=[hbm] * 4,
        out_specs=vmem,
        scratch_shapes=[
            pltpu.VMEM(volume.shape, jnp.int32),
            pltpu.VMEM(transfer_table.shape, jnp.float32),
            pltpu.SMEM(depth_rank.shape, jnp.int32),
            pltpu.SMEM(footprint.shape, jnp.int32),
            pltpu.SemaphoreType.DMA((4,)),
            pltpu.VMEM((depth, rows, lanes), jnp.float32),
            pltpu.VMEM((3, depth, rows, lanes), jnp.float32),
            pltpu.VMEM((4, 8, lanes), jnp.float32),
            pltpu.VMEM((2, rows, lanes), jnp.float32),
            pltpu.VMEM((2, depth, lanes), jnp.float32),
            pltpu.VMEM((2, 8, lanes), jnp.float32),
            pltpu.VMEM((n, rows, lanes), jnp.float32),
            pltpu.VMEM((n, 3, rows, lanes), jnp.float32),
            pltpu.SemaphoreType.DMA((3, 2)),
            pltpu.SemaphoreType.DMA((3, 2)),
            pltpu.SemaphoreType.DMA((n,)),
            pltpu.SemaphoreType.DMA((n,)),
            pltpu.SemaphoreType.DMA((n,)),
            pltpu.SemaphoreType.DMA((n,)),
        ],
        compiler_params=pltpu.CompilerParams(collective_id=0, has_side_effects=True),
        name="raycast",
    )(volume, transfer_table, depth_rank, footprint)


def solution(mesh):
    placed = (P("gx", "gy", "gz"), P(), P(), P("gx", "gy", "gz", None))
    sizes = tuple(mesh.shape[a] for a in AXES)
    return jax.shard_map(
        functools.partial(on_device, sizes), mesh=mesh, in_specs=placed,
        out_specs=P(None, "gy", "gz"), check_vma=False,
    )
```

```python
import functools

import jax
import jax.numpy as jnp
from jax import lax
from jax.experimental import pallas as pl
from jax.experimental.pallas import tpu as pltpu
from jax.sharding import PartitionSpec as P

LIGHT = (1.0 / 3.0, 2.0 / 3.0, 2.0 / 3.0)
AXES = ("gx", "gy", "gz")
MESH = pl.DeviceIdType.MESH


def lookup(table_row, index, lanes):
    entries = table_row.shape[1]
    low = index & (lanes - 1)
    found = None
    for part in range(entries // lanes):
        piece = jnp.broadcast_to(table_row[:, part * lanes:(part + 1) * lanes], index.shape)
        got = jnp.take_along_axis(piece, low, axis=1, mode="promise_in_bounds")
        found = got if found is None else jnp.where(index >= part * lanes, got, found)
    return found


def kernel(sizes, vol_hbm, table_hbm, rank_hbm, foot_hbm, out_ref,
           vol_ref, table_ref, rank_ref, foot_ref, load_sem, dens, wemit, inner, edge, xh, yh, zh, alphas, colours,
           halo_send, halo_recv, a_send, a_recv, c_send, c_recv):
    n, ny, nz = sizes
    depth, rows, lanes = vol_ref.shape
    extent = 4.0 / (depth * n)
    me = [lax.axis_index(a) for a in AXES]
    ix = me[0]

    barrier = pltpu.get_barrier_semaphore()
    for off in range(1, n):
        pl.semaphore_signal(barrier, inc=1, device_id={"gx": lax.rem(ix + off, n)}, device_id_type=MESH)
    for a in (1, 2):
        if sizes[a] > 1:
            @pl.when(me[a] > 0)
            def _():
                pl.semaphore_signal(barrier, inc=1, device_id={AXES[a]: me[a] - 1}, device_id_type=MESH)

            @pl.when(me[a] < sizes[a] - 1)
            def _():
                pl.semaphore_signal(barrier, inc=1, device_id={AXES[a]: me[a] + 1}, device_id_type=MESH)

    loads = [
        pltpu.make_async_copy(src, dst, load_sem.at[i])
        for i, (src, dst) in enumerate((
            (vol_hbm, vol_ref), (table_hbm, table_ref), (foot_hbm, foot_ref), (rank_hbm, rank_ref)
        ))
    ]
    for load in loads:
        load.start()
    loads[0].wait()
    loads[1].wait()

    lane = lax.broadcasted_iota(jnp.int32, (8, lanes), 1)
    vol = vol_ref[...].reshape(depth * rows, lanes)
    d_all = lookup(table_ref[3:4, :], vol, lanes)
    d3 = d_all.reshape(depth, rows, lanes)
    dens[...] = d3
    edge[0] = d3[:, 0, :]
    edge[1] = d3[:, rows - 1, :]
    first = jnp.zeros((8, lanes), jnp.float32)
    last = jnp.zeros((8, lanes), jnp.float32)
    groups = depth * rows // 8
    for v in range(groups):
        piece = d_all[v * 8:(v + 1) * 8]
        to_last = (2 * v + 1) % lanes
        to_first = (2 * v - 1) % lanes
        last = jnp.where(lane == 2 * v, pltpu.roll(piece, to_last, 1) if to_last else piece, last)
        first = jnp.where(lane == to_first, pltpu.roll(piece, to_first, 1) if to_first else piece, first)
    edge[2] = first
    edge[3] = last

    sources = (
        (dens.at[0], dens.at[depth - 1]),
        (edge.at[0], edge.at[1]),
        (edge.at[2], edge.at[3]),
    )
    halos = (xh, yh, zh)

    def halo_copy(a, upward):
        slot = 0 if upward else 1
        return pltpu.make_async_remote_copy(
            src_ref=sources[a][1 if upward else 0],
            dst_ref=halos[a].at[slot],
            send_sem=halo_send.at[a, slot],
            recv_sem=halo_recv.at[a, slot],
            device_id={AXES[a]: me[a] + (1 if upward else -1)},
            device_id_type=MESH,
        )

    greeted = n - 1
    for a in (1, 2):
        greeted = greeted + lax.min(me[a], 1) + lax.min(sizes[a] - 1 - me[a], 1)
    pl.semaphore_wait(barrier, greeted)

    for a in (1, 2, 0):
        @pl.when(me[a] < sizes[a] - 1)
        def _():
            halo_copy(a, True).start()

        @pl.when(me[a] == 0)
        def _():
            halos[a][0] = jnp.zeros(halos[a].shape[1:], jnp.float32)

        @pl.when(me[a] > 0)
        def _():
            halo_copy(a, False).start()

        @pl.when(me[a] == sizes[a] - 1)
        def _():
            halos[a][1] = jnp.zeros(halos[a].shape[1:], jnp.float32)

    loads[2].wait()
    row_no = lax.broadcasted_iota(jnp.int32, (rows, lanes), 0)
    lane_no = lax.broadcasted_iota(jnp.int32, (rows, lanes), 1)
    inside = (
        (row_no >= foot_ref[0, 0, 0, 0])
        & (row_no < foot_ref[0, 0, 0, 1])
        & (lane_no >= foot_ref[0, 0, 0, 2])
        & (lane_no < foot_ref[0, 0, 0, 3])
    )

    transmit = jnp.ones((rows, lanes), jnp.float32)
    weights = []
    for x in range(depth):
        sample = 1.0 - jnp.exp(-extent * d3[x])
        weights.append(transmit * sample)
        transmit = transmit * (1.0 - sample)
    alphas[ix] = jnp.where(inside, 1.0 - transmit, 0.0)

    def image_copy(buf, off, s_sem, r_sem):
        return pltpu.make_async_remote_copy(
            src_ref=buf.at[ix],
            dst_ref=buf.at[ix],
            send_sem=s_sem.at[off],
            recv_sem=r_sem.at[off],
            device_id={"gx": lax.rem(ix + off, n)},
            device_id_type=MESH,
        )

    def send_images(buf, s_sem, r_sem):
        for far in range(n - 1, 0, -1):
            @pl.when(ix + far < n)
            def _():
                image_copy(buf, far, s_sem, r_sem).start()

            @pl.when(ix - far >= 0)
            def _():
                image_copy(buf, n - far, s_sem, r_sem).start()

    send_images(alphas, a_send, a_recv)

    for c in range(3):
        emit = lookup(table_ref[c:c + 1, :], vol, lanes).reshape(depth, rows, lanes)
        for x in range(depth):
            wemit[c, x] = weights[x] * emit[x]

    per = rows // 8
    for x in range(depth):
        d = d3[x]
        up = jnp.where(row_no == 0, 0.0, pltpu.roll(d, 1, 0))
        down = jnp.where(row_no == rows - 1, 0.0, pltpu.roll(d, rows - 1, 0))
        inner[0, x] = 0.5 * (down - up)
        left = jnp.where(lane_no == 0, 0.0, pltpu.roll(d, 1, 1))
        right = jnp.where(lane_no == lanes - 1, 0.0, pltpu.roll(d, lanes - 1, 1))
        inner[1, x] = 0.5 * (right - left)
    line = lax.broadcasted_iota(jnp.int32, (8, lanes), 0)
    on_side = (lane == 0) | (lane == lanes - 1)

    for a in range(3):
        @pl.when(me[a] > 0)
        def _():
            halo_copy(a, True).wait_recv()

        @pl.when(me[a] < sizes[a] - 1)
        def _():
            halo_copy(a, False).wait_recv()

    sides = 0.5 * (zh[1] - zh[0])
    half_up = 0.5 * yh[0]
    half_down = 0.5 * yh[1]
    layers = [xh.at[0]] + [dens.at[x] for x in range(depth)] + [xh.at[1]]
    colour = [[None] * per for _ in range(3)]
    for x in range(depth):
        for h in range(per):
            at = pl.ds(h * 8, 8)
            v = x * per + h
            g_x = 0.5 * (layers[x + 2][at, :] - layers[x][at, :])
            g_y = inner[0, x, at, :]
            if h == 0:
                g_y = jnp.where(line == 0, g_y - half_up[x:x + 1, :], g_y)
            if h == per - 1:
                g_y = jnp.where(line == 7, g_y + half_down[x:x + 1, :], g_y)
            side = pltpu.roll(sides, lanes - 2 * v, 1) if v else sides
            g_z = inner[1, x, at, :]
            g_z = jnp.where(on_side, g_z + side, g_z)
            facing = jnp.abs(g_x * LIGHT[0] + g_y * LIGHT[1] + g_z * LIGHT[2]) * lax.rsqrt(
                1.0 + (g_x * g_x + g_y * g_y + g_z * g_z)
            )
            shade = 0.35 + 0.65 * facing
            for c in range(3):
                term = wemit[c, x, at, :] * shade
                colour[c][h] = term if x == 0 else colour[c][h] + term
    colour = [jnp.concatenate(c, axis=0) for c in colour]
    for c in range(3):
        colours[ix, c] = jnp.where(inside, colour[c], 0.0)

    send_images(colours, c_send, c_recv)

    loads[3].wait()
    order = []
    for p in range(n):
        at = 0
        for i in range(n):
            at = jnp.where(rank_ref[i] == p, i, at)
        order.append(at)

    for off in range(1, n):
        image_copy(alphas, off, a_send, a_recv).wait_recv()
    covers = []
    alpha = jnp.zeros((rows, lanes), jnp.float32)
    for p in range(n):
        covers.append(1.0 - alpha)
        alpha = alpha + covers[p] * alphas[order[p]]
    out_ref[3] = alpha
    for a in range(3):
        @pl.when(me[a] < sizes[a] - 1)
        def _():
            halo_copy(a, True).wait_send()

        @pl.when(me[a] > 0)
        def _():
            halo_copy(a, False).wait_send()
    for off in range(1, n):
        image_copy(alphas, off, a_send, a_recv).wait_send()

    for off in range(1, n):
        image_copy(colours, off, c_send, c_recv).wait_recv()
    total = [None] * 3
    for p in range(n):
        for c in range(3):
            term = covers[p] * colours[order[p], c]
            total[c] = term if p == 0 else total[c] + term
    for c in range(3):
        out_ref[c] = total[c]
    for off in range(1, n):
        image_copy(colours, off, c_send, c_recv).wait_send()


def on_device(sizes, volume, transfer_table, depth_rank, footprint):
    depth, rows, lanes = volume.shape
    n = sizes[0]
    vmem = pl.BlockSpec(memory_space=pltpu.VMEM)
    hbm = pl.BlockSpec(memory_space=pl.ANY)
    return pl.pallas_call(
        functools.partial(kernel, sizes),
        out_shape=pltpu.VMEM((4, rows, lanes), jnp.float32),
        in_specs=[hbm] * 4,
        out_specs=vmem,
        scratch_shapes=[
            pltpu.VMEM(volume.shape, jnp.int32),
            pltpu.VMEM(transfer_table.shape, jnp.float32),
            pltpu.SMEM(depth_rank.shape, jnp.int32),
            pltpu.SMEM(footprint.shape, jnp.int32),
            pltpu.SemaphoreType.DMA((4,)),
            pltpu.VMEM((depth, rows, lanes), jnp.float32),
            pltpu.VMEM((3, depth, rows, lanes), jnp.float32),
            pltpu.VMEM((2, depth, rows, lanes), jnp.float32),
            pltpu.VMEM((4, 8, lanes), jnp.float32),
            pltpu.VMEM((2, rows, lanes), jnp.float32),
            pltpu.VMEM((2, depth, lanes), jnp.float32),
            pltpu.VMEM((2, 8, lanes), jnp.float32),
            pltpu.VMEM((n, rows, lanes), jnp.float32),
            pltpu.VMEM((n, 3, rows, lanes), jnp.float32),
            pltpu.SemaphoreType.DMA((3, 2)),
            pltpu.SemaphoreType.DMA((3, 2)),
            pltpu.SemaphoreType.DMA((n,)),
            pltpu.SemaphoreType.DMA((n,)),
            pltpu.SemaphoreType.DMA((n,)),
            pltpu.SemaphoreType.DMA((n,)),
        ],
        compiler_params=pltpu.CompilerParams(collective_id=0, has_side_effects=True),
        name="raycast",
    )(volume, transfer_table, depth_rank, footprint)


def solution(mesh):
    placed = (P("gx", "gy", "gz"), P(), P(), P("gx", "gy", "gz", None))
    sizes = tuple(mesh.shape[a] for a in AXES)
    return jax.shard_map(
        functools.partial(on_device, sizes), mesh=mesh, in_specs=placed,
        out_specs=P(None, "gy", "gz"), check_vma=False,
    )
```

```python
import functools

import jax
import jax.numpy as jnp
from jax import lax
from jax.experimental import pallas as pl
from jax.experimental.pallas import tpu as pltpu
from jax.sharding import PartitionSpec as P

LIGHT = (1.0 / 3.0, 2.0 / 3.0, 2.0 / 3.0)
AXES = ("gx", "gy", "gz")
MESH = pl.DeviceIdType.MESH


def lookup(table_row, index, lanes):
    entries = table_row.shape[1]
    low = index & (lanes - 1)
    found = None
    for part in range(entries // lanes):
        piece = jnp.broadcast_to(table_row[:, part * lanes:(part + 1) * lanes], index.shape)
        got = jnp.take_along_axis(piece, low, axis=1, mode="promise_in_bounds")
        found = got if found is None else jnp.where(index >= part * lanes, got, found)
    return found


def kernel(sizes, vol_hbm, table_hbm, rank_hbm, foot_hbm, out_ref,
           vol_ref, table_ref, rank_ref, foot_ref, load_sem, dens, wemit, inner, edge, xh, yh, zh, alphas, colours,
           halo_send, halo_recv, a_send, a_recv, c_send, c_recv):
    n, ny, nz = sizes
    depth, rows, lanes = vol_ref.shape
    extent = 4.0 / (depth * n)
    me = [lax.axis_index(a) for a in AXES]
    ix = me[0]

    barrier = pltpu.get_barrier_semaphore()
    for off in range(1, n):
        pl.semaphore_signal(barrier, inc=1, device_id={"gx": lax.rem(ix + off, n)}, device_id_type=MESH)
    for a in (1, 2):
        if sizes[a] > 1:
            @pl.when(me[a] > 0)
            def _():
                pl.semaphore_signal(barrier, inc=1, device_id={AXES[a]: me[a] - 1}, device_id_type=MESH)

            @pl.when(me[a] < sizes[a] - 1)
            def _():
                pl.semaphore_signal(barrier, inc=1, device_id={AXES[a]: me[a] + 1}, device_id_type=MESH)

    loads = [
        pltpu.make_async_copy(src, dst, load_sem.at[i])
        for i, (src, dst) in enumerate((
            (vol_hbm, vol_ref), (table_hbm, table_ref), (foot_hbm, foot_ref), (rank_hbm, rank_ref)
        ))
    ]
    for load in loads:
        load.start()
    loads[0].wait()
    loads[1].wait()

    lane = lax.broadcasted_iota(jnp.int32, (8, lanes), 1)
    vol = vol_ref[...].reshape(depth * rows, lanes)
    d_all = lookup(table_ref[3:4, :], vol, lanes)
    d3 = d_all.reshape(depth, rows, lanes)
    dens[...] = d3
    edge[0] = d3[:, 0, :]
    edge[1] = d3[:, rows - 1, :]
    first = jnp.zeros((8, lanes), jnp.float32)
    last = jnp.zeros((8, lanes), jnp.float32)
    groups = depth * rows // 8
    for v in range(groups):
        piece = d_all[v * 8:(v + 1) * 8]
        to_last = (2 * v + 1) % lanes
        to_first = (2 * v - 1) % lanes
        last = jnp.where(lane == 2 * v, pltpu.roll(piece, to_last, 1) if to_last else piece, last)
        first = jnp.where(lane == to_first, pltpu.roll(piece, to_first, 1) if to_first else piece, first)
    edge[2] = first
    edge[3] = last

    sources = (
        (dens.at[0], dens.at[depth - 1]),
        (edge.at[0], edge.at[1]),
        (edge.at[2], edge.at[3]),
    )
    halos = (xh, yh, zh)

    def halo_copy(a, upward):
        slot = 0 if upward else 1
        return pltpu.make_async_remote_copy(
            src_ref=sources[a][1 if upward else 0],
            dst_ref=halos[a].at[slot],
            send_sem=halo_send.at[a, slot],
            recv_sem=halo_recv.at[a, slot],
            device_id={AXES[a]: me[a] + (1 if upward else -1)},
            device_id_type=MESH,
        )

    for a in range(3):
        @pl.when(me[a] == 0)
        def _():
            halos[a][0] = jnp.zeros(halos[a].shape[1:], jnp.float32)

        @pl.when(me[a] == sizes[a] - 1)
        def _():
            halos[a][1] = jnp.zeros(halos[a].shape[1:], jnp.float32)

    loads[2].wait()
    row_no = lax.broadcasted_iota(jnp.int32, (rows, lanes), 0)
    lane_no = lax.broadcasted_iota(jnp.int32, (rows, lanes), 1)
    inside = (
        (row_no >= foot_ref[0, 0, 0, 0])
        & (row_no < foot_ref[0, 0, 0, 1])
        & (lane_no >= foot_ref[0, 0, 0, 2])
        & (lane_no < foot_ref[0, 0, 0, 3])
    )

    transmit = jnp.ones((rows, lanes), jnp.float32)
    weights = []
    for x in range(depth):
        sample = 1.0 - jnp.exp(-extent * d3[x])
        weights.append(transmit * sample)
        transmit = transmit * (1.0 - sample)
    alphas[ix] = jnp.where(inside, 1.0 - transmit, 0.0)

    greeted = n - 1
    for a in (1, 2):
        greeted = greeted + lax.min(me[a], 1) + lax.min(sizes[a] - 1 - me[a], 1)
    pl.semaphore_wait(barrier, greeted)

    for a in (1, 2, 0):
        @pl.when(me[a] < sizes[a] - 1)
        def _():
            halo_copy(a, True).start()

        @pl.when(me[a] > 0)
        def _():
            halo_copy(a, False).start()

    def image_copy(buf, off, s_sem, r_sem):
        return pltpu.make_async_remote_copy(
            src_ref=buf.at[ix],
            dst_ref=buf.at[ix],
            send_sem=s_sem.at[off],
            recv_sem=r_sem.at[off],
            device_id={"gx": lax.rem(ix + off, n)},
            device_id_type=MESH,
        )

    def send_images(buf, s_sem, r_sem):
        for far in range(n - 1, 0, -1):
            @pl.when(ix + far < n)
            def _():
                image_copy(buf, far, s_sem, r_sem).start()

            @pl.when(ix - far >= 0)
            def _():
                image_copy(buf, n - far, s_sem, r_sem).start()

    send_images(alphas, a_send, a_recv)

    for c in range(3):
        emit = lookup(table_ref[c:c + 1, :], vol, lanes).reshape(depth, rows, lanes)
        for x in range(depth):
            wemit[c, x] = weights[x] * emit[x]

    per = rows // 8
    for x in range(depth):
        d = d3[x]
        up = jnp.where(row_no == 0, 0.0, pltpu.roll(d, 1, 0))
        down = jnp.where(row_no == rows - 1, 0.0, pltpu.roll(d, rows - 1, 0))
        inner[0, x] = 0.5 * (down - up)
        left = jnp.where(lane_no == 0, 0.0, pltpu.roll(d, 1, 1))
        right = jnp.where(lane_no == lanes - 1, 0.0, pltpu.roll(d, lanes - 1, 1))
        inner[1, x] = 0.5 * (right - left)
    line = lax.broadcasted_iota(jnp.int32, (8, lanes), 0)
    on_side = (lane == 0) | (lane == lanes - 1)

    for a in range(3):
        @pl.when(me[a] > 0)
        def _():
            halo_copy(a, True).wait_recv()

        @pl.when(me[a] < sizes[a] - 1)
        def _():
            halo_copy(a, False).wait_recv()

    sides = 0.5 * (zh[1] - zh[0])
    half_up = 0.5 * yh[0]
    half_down = 0.5 * yh[1]
    layers = [xh.at[0]] + [dens.at[x] for x in range(depth)] + [xh.at[1]]
    colour = [[None] * per for _ in range(3)]
    for x in range(depth):
        for h in range(per):
            at = pl.ds(h * 8, 8)
            v = x * per + h
            g_x = 0.5 * (layers[x + 2][at, :] - layers[x][at, :])
            g_y = inner[0, x, at, :]
            if h == 0:
                g_y = jnp.where(line == 0, g_y - half_up[x:x + 1, :], g_y)
            if h == per - 1:
                g_y = jnp.where(line == 7, g_y + half_down[x:x + 1, :], g_y)
            side = pltpu.roll(sides, lanes - 2 * v, 1) if v else sides
            g_z = inner[1, x, at, :]
            g_z = jnp.where(on_side, g_z + side, g_z)
            facing = jnp.abs(g_x * LIGHT[0] + g_y * LIGHT[1] + g_z * LIGHT[2]) * lax.rsqrt(
                1.0 + (g_x * g_x + g_y * g_y + g_z * g_z)
            )
            shade = 0.35 + 0.65 * facing
            for c in range(3):
                term = wemit[c, x, at, :] * shade
                colour[c][h] = term if x == 0 else colour[c][h] + term
    colour = [jnp.concatenate(c, axis=0) for c in colour]
    for c in range(3):
        colours[ix, c] = jnp.where(inside, colour[c], 0.0)

    send_images(colours, c_send, c_recv)

    loads[3].wait()
    order = []
    for p in range(n):
        at = 0
        for i in range(n):
            at = jnp.where(rank_ref[i] == p, i, at)
        order.append(at)

    for off in range(1, n):
        image_copy(alphas, off, a_send, a_recv).wait_recv()
    covers = []
    alpha = jnp.zeros((rows, lanes), jnp.float32)
    for p in range(n):
        covers.append(1.0 - alpha)
        alpha = alpha + covers[p] * alphas[order[p]]
    out_ref[3] = alpha
    for a in range(3):
        @pl.when(me[a] < sizes[a] - 1)
        def _():
            halo_copy(a, True).wait_send()

        @pl.when(me[a] > 0)
        def _():
            halo_copy(a, False).wait_send()
    for off in range(1, n):
        image_copy(alphas, off, a_send, a_recv).wait_send()

    for off in range(1, n):
        image_copy(colours, off, c_send, c_recv).wait_recv()
    total = [None] * 3
    for p in range(n):
        for c in range(3):
            term = covers[p] * colours[order[p], c]
            total[c] = term if p == 0 else total[c] + term
    for c in range(3):
        out_ref[c] = total[c]
    for off in range(1, n):
        image_copy(colours, off, c_send, c_recv).wait_send()


def on_device(sizes, volume, transfer_table, depth_rank, footprint):
    depth, rows, lanes = volume.shape
    n = sizes[0]
    vmem = pl.BlockSpec(memory_space=pltpu.VMEM)
    hbm = pl.BlockSpec(memory_space=pl.ANY)
    return pl.pallas_call(
        functools.partial(kernel, sizes),
        out_shape=pltpu.VMEM((4, rows, lanes), jnp.float32),
        in_specs=[hbm] * 4,
        out_specs=vmem,
        scratch_shapes=[
            pltpu.VMEM(volume.shape, jnp.int32),
            pltpu.VMEM(transfer_table.shape, jnp.float32),
            pltpu.SMEM(depth_rank.shape, jnp.int32),
            pltpu.SMEM(footprint.shape, jnp.int32),
            pltpu.SemaphoreType.DMA((4,)),
            pltpu.VMEM((depth, rows, lanes), jnp.float32),
            pltpu.VMEM((3, depth, rows, lanes), jnp.float32),
            pltpu.VMEM((2, depth, rows, lanes), jnp.float32),
            pltpu.VMEM((4, 8, lanes), jnp.float32),
            pltpu.VMEM((2, rows, lanes), jnp.float32),
            pltpu.VMEM((2, depth, lanes), jnp.float32),
            pltpu.VMEM((2, 8, lanes), jnp.float32),
            pltpu.VMEM((n, rows, lanes), jnp.float32),
            pltpu.VMEM((n, 3, rows, lanes), jnp.float32),
            pltpu.SemaphoreType.DMA((3, 2)),
            pltpu.SemaphoreType.DMA((3, 2)),
            pltpu.SemaphoreType.DMA((n,)),
            pltpu.SemaphoreType.DMA((n,)),
            pltpu.SemaphoreType.DMA((n,)),
            pltpu.SemaphoreType.DMA((n,)),
        ],
        compiler_params=pltpu.CompilerParams(collective_id=0, has_side_effects=True),
        name="raycast",
    )(volume, transfer_table, depth_rank, footprint)


def solution(mesh):
    placed = (P("gx", "gy", "gz"), P(), P(), P("gx", "gy", "gz", None))
    sizes = tuple(mesh.shape[a] for a in AXES)
    return jax.shard_map(
        functools.partial(on_device, sizes), mesh=mesh, in_specs=placed,
        out_specs=P(None, "gy", "gz"), check_vma=False,
    )
```
